32 devices in a mesh: member: 8 (over y, x, core), lat: 4 (over z).
Axes of the slice: x: 2, y: 2, z: 4, core: 2. Of those that a mesh axis runs over, the one named last changes fastest.
Arguments:
- ensemble: float32 [16, 3, 1, 32, 1440], P('member', None, None, 'lat'), may hold values from -6 to 6
- observation: float32 [3, 1, 32, 1440], P(None, None, 'lat'), may hold values from -6 to 6
- valid_mask: int32 [16], P('member'), may hold values from 0 to 1, as said below
- band_start: int32 [4], P('lat'), may hold values from 0 to 713
Outputs:
- crps_field: float32 [3, 1, 32, 1440], P(None, None, ('lat', 'member'))
- score_table: float32 [3, 1], replicated
The draws below stay inside these ranges and needn't reach their ends.
Inputs may be any that keep to these rules, and one draw needn't show every extreme that they name: `valid_mask`: exactly 13 entries are 1, at positions drawn afresh.
All inputs are finite; a program needn't handle non-finite values.
Results may differ from the reference program's by a relative error of at most 0.0001.
Values sent between devices are 32-bit elements; how exact they have to be, the bound alone decides.
A program may use at most 64 MiB of HBM per device.

```python
import math
import jax
import jax.numpy as jnp
from jax import lax

GRID_LAT = 721
GRID_LON = 1440
VARS = 3
LEADS = 1
LAT_DEV = 8
MEMBERS = 16
VALID = 13
LAT = 32
N_LAT = 4


def draw_valid_mask(key, part):
    shuffled = jax.random.permutation(jax.random.fold_in(key, 17), MEMBERS)
    return (shuffled < VALID).astype(jnp.int32)


def touch_ends(drawn, key, low, top_value):
    dims = drawn.shape
    spot = [jax.random.randint(jax.random.fold_in(key, axis), (), 0, dims[axis]) for axis in range(len(dims))]
    drawn = drawn.at[tuple(spot)].set(low)
    longest = dims.index(max(dims))
    spot[longest] = (spot[longest] + 1) % dims[longest]
    return drawn.at[tuple(spot)].set(top_value)


def steps_of(stream_key, shape, pieces, low, high):
    gain = 1.0
    for dim, shards_of in pieces:
        steps = jax.random.uniform(jax.random.fold_in(jax.random.fold_in(stream_key, 6), dim), (shards_of,), jnp.float32, low / len(pieces), high / len(pieces))
        gain = gain * jnp.repeat(jnp.exp(steps), shape[dim] // shards_of).reshape((-1,) + (1,) * (len(shape) - 1 - dim))
    return gain


def scatter_about(own_key, extent, scale, bound, split=(), kind=jnp.bfloat16):
    values = scale * jax.random.normal(own_key, extent, jnp.float32)
    if split:
        values = values * steps_of(own_key, extent, split, -0.22, 0.18)
    return jnp.clip(values, -bound, bound).astype(kind)


def setup_inputs(seed: int = 0) -> dict:
    arg_keys = jax.random.split(jax.random.key(seed), 5)
    return {
        "ensemble": scatter_about(arg_keys[0], (MEMBERS, VARS, LEADS, LAT, GRID_LON), 1.0, 6.0, ((0, 8), (3, 4)), jnp.float32),
        "observation": scatter_about(arg_keys[1], (VARS, LEADS, LAT, GRID_LON), 1.0, 6.0, ((2, 4),), jnp.float32),
        "valid_mask": draw_valid_mask(jax.random.fold_in(arg_keys[4], 71), 0),
        "band_start": touch_ends(jax.random.randint(arg_keys[3], (N_LAT,), 0, GRID_LAT - LAT_DEV + 1), jax.random.fold_in(arg_keys[3], 1), 0, GRID_LAT - LAT_DEV).astype(jnp.int32),
    }


def reference(ensemble, observation, valid_mask, band_start):
    member_flags = valid_mask.astype(jnp.float32)
    valid_count = jnp.sum(member_flags)
    flag_column = member_flags[:, None, None, None, None]
    skill_term = jnp.sum(flag_column * jnp.abs(ensemble - observation[None]), axis=0)

    def accumulate(running_sum, block_item):
        member_slab, member_flag = block_item
        distance = jnp.sum(flag_column * jnp.abs(member_slab[None] - ensemble), axis=0)
        return running_sum + member_flag * distance, None

    spread, unused = lax.scan(accumulate, jnp.zeros(observation.shape, jnp.float32), (ensemble, member_flags))
    crps_field = skill_term / valid_count - spread / (2.0 * valid_count * (valid_count - 1.0))
    row_index = (band_start[:, None] + jnp.arange(LAT_DEV, dtype=jnp.int32)[None, :]).reshape(-1).astype(jnp.float32)
    weight = jnp.cos((90.0 - row_index * 180.0 / (GRID_LAT - 1)) * math.pi / 180.0)
    score_table = jnp.sum(crps_field * weight[:, None], axis=(2, 3)) / (N_LAT * LAT_DEV * GRID_LON)
    return (crps_field, score_table)
```

```python
import functools
import math

import jax
import jax.numpy as jnp
from jax import lax
from jax.experimental import pallas as pl
from jax.experimental.pallas import tpu as pltpu
from jax.sharding import PartitionSpec as P

GRID_LAT = 721
GRID_LON = 1440
LANES = 128
SUBLANES = 8
FILL = 1e30
MESH = pl.DeviceIdType.MESH


def round_up(value, step):
    return (value + step - 1) // step * step


def sort_pairs(count):
    pairs = []
    p = 1
    while p < count:
        k = p
        while k >= 1:
            for j in range(k % p, count - k, 2 * k):
                for i in range(min(k, count - j - k)):
                    if (i + j) // (2 * p) == (i + j + k) // (2 * p):
                        pairs.append((i + j, i + j + k))
            k //= 2
        p *= 2
    return pairs


def other(me, k, n):
    partner, bit = 0, 1
    while bit < n:
        here = (me // bit) % 2
        partner = partner + bit * (1 - here if k & bit else here)
        bit *= 2
    return partner


def chunk_of(ref, index, low, lon):
    wide = min(LANES, lon - low)
    value = ref[index + (pl.ds(low, wide),)]
    if wide < LANES:
        value = jnp.concatenate([value, jnp.zeros((SUBLANES, LANES - wide), value.dtype)], axis=1)
    return value


def kernel(
    n, nz, ens_ref, obs_ref, mask_ref, band_ref, field_ref, table_ref,
    ens_v, obs_v, packet, obs_rows, gathered, field_v, partials,
    load_sem, send_sem, recv_sem, psend_sem, precv_sem,
):
    held, variables, leads, rows, lon = ens_ref.shape
    units = variables * leads
    chunks = round_up(lon, LANES) // LANES
    lines = units * chunks
    group = round_up(lines + 1, SUBLANES)
    pitch = packet.shape[0] // n
    slots = n * held
    total = n * nz
    me = lax.axis_index("member")
    band = lax.axis_index("lat")
    mine = band * n + me

    loads = [
        pltpu.make_async_copy(ens_ref.at[m], ens_v.at[m], load_sem.at[m]) for m in range(held)
    ]
    loads.append(pltpu.make_async_copy(obs_ref, obs_v, load_sem.at[held]))
    for load in loads:
        load.start()

    barrier = pltpu.get_barrier_semaphore()
    for k in range(1, total):
        far = lax.rem(mine + k, total)
        pl.semaphore_signal(
            barrier, inc=1, device_id={"member": far % n, "lat": far // n}, device_id_type=MESH
        )

    for m in range(held):
        loads[m].wait()
        flag = jnp.full((SUBLANES, LANES), mask_ref[m], jnp.int32)
        keep = flag != 0
        for block in range(0, rows, SUBLANES):
            base = block * pitch + m * group
            for v in range(variables):
                for t in range(leads):
                    for c in range(chunks):
                        value = chunk_of(ens_v, (m, v, t, pl.ds(block, SUBLANES)), c * LANES, lon)
                        line = (v * leads + t) * chunks + c
                        packet[pl.ds(base + line, SUBLANES, stride=pitch), :] = jnp.where(
                            keep, value, FILL
                        )
            for line in range(lines, group):
                packet[pl.ds(base + line, SUBLANES, stride=pitch), :] = flag.astype(jnp.float32)

    pl.semaphore_wait(barrier, total - 1)

    sends = []
    for k in sorted(range(1, n), key=lambda k: (-bin(k // 2).count("1"), k)):
        far = other(me, k, n)
        sends.append(
            pltpu.make_async_remote_copy(
                src_ref=packet.at[pl.ds(pl.multiple_of(far * pitch, SUBLANES), held * group)],
                dst_ref=gathered.at[
                    pl.ds(pl.multiple_of(me * held * group, SUBLANES), held * group)
                ],
                send_sem=send_sem.at[k],
                recv_sem=recv_sem.at[k],
                device_id={"member": far, "lat": band},
                device_id_type=MESH,
            )
        )
        sends[-1].start()

    loads[held].wait()
    for block in range(0, rows, SUBLANES):
        for v in range(variables):
            for t in range(leads):
                for c in range(chunks):
                    line = (v * leads + t) * chunks + c
                    obs_rows[pl.ds(block * group + line, SUBLANES, stride=group), :] = chunk_of(
                        obs_v, (v, t, pl.ds(block, SUBLANES)), c * LANES, lon
                    )
    gathered[pl.ds(pl.multiple_of(me * held * group, SUBLANES), held * group), :] = packet[
        pl.ds(pl.multiple_of(me * pitch, SUBLANES), held * group), :
    ]
    row_number = jnp.full((1, LANES), band_ref[0] + me, jnp.int32).astype(jnp.float32)
    weight = jnp.cos((90.0 - row_number * 180.0 / (GRID_LAT - 1)) * math.pi / 180.0)

    for send in sends:
        send.wait_recv()

    flags = jnp.concatenate(
        [gathered[pl.ds(s * group + lines, 1), :] for s in range(slots)], axis=0
    )
    count = jnp.broadcast_to(jnp.sum(flags, axis=0, keepdims=True), (SUBLANES, LANES))
    per_one = 1.0 / count
    per_pair = per_one / (count - 1.0)
    skill_weight, spread_weight = [], []
    for i in range(slots):
        counted = i < count
        skill_weight.append(jnp.where(counted, per_one, 0.0))
        spread_weight.append(jnp.where(counted, (2.0 * i + 1.0 - count) * per_pair, 0.0))

    network = sort_pairs(slots)
    sums = [None] * units
    blocks = []
    for j in range(0, group, SUBLANES):
        x = [gathered[pl.ds(s * group + j, SUBLANES), :] for s in range(slots)]
        for a, b in network:
            x[a], x[b] = jnp.minimum(x[a], x[b]), jnp.maximum(x[a], x[b])
        truth = obs_rows[pl.ds(pl.multiple_of(me * group + j, SUBLANES), SUBLANES), :]
        score = None
        for i in range(slots):
            term = skill_weight[i] * jnp.abs(x[i] - truth) - spread_weight[i] * x[i]
            score = term if score is None else score + term
        blocks.append(score)
        line = j + lax.broadcasted_iota(jnp.int32, (SUBLANES, LANES), 0)
        for u in range(units):
            low, high = u * chunks, (u + 1) * chunks
            if low < j + SUBLANES and j < high:
                part = jnp.where((line >= low) & (line < high), score, 0.0)
                sums[u] = part if sums[u] is None else sums[u] + part

    lane = lax.broadcasted_iota(jnp.int32, (1, LANES), 1)
    row = jnp.zeros((1, LANES), jnp.float32)
    for u in range(units):
        one = jnp.sum(jnp.sum(sums[u], axis=0, keepdims=True), axis=1, keepdims=True)
        row = jnp.where(lane == u, one, row)
    partials[pl.ds(mine, 1), :] = row * weight

    for send in sends:
        send.wait_send()
    for line in range(lines):
        u, c = line // chunks, line % chunks
        wide = min(LANES, lon - c * LANES)
        score = blocks[line // SUBLANES]
        at = line % SUBLANES
        field_v[u // leads, u % leads, :, pl.ds(c * LANES, wide)] = score[at : at + 1, :wide]
    out = pltpu.make_async_copy(field_v, field_ref, load_sem.at[0])
    out.start()

    shares = []
    for k in range(1, total):
        far = lax.rem(mine + k, total)
        shares.append(
            pltpu.make_async_remote_copy(
                src_ref=partials.at[pl.ds(mine, 1)],
                dst_ref=partials.at[pl.ds(mine, 1)],
                send_sem=psend_sem.at[k],
                recv_sem=precv_sem.at[k],
                device_id={"member": far % n, "lat": far // n},
                device_id_type=MESH,
            )
        )
        shares[-1].start()
    for share in shares:
        share.wait_recv()
    summed = jnp.sum(partials[...], axis=0, keepdims=True)
    spot = lax.broadcasted_iota(jnp.int32, (units, LANES), 0)
    across = lax.broadcasted_iota(jnp.int32, (units, LANES), 1)
    diagonal = jnp.where(spot == across, jnp.broadcast_to(summed, (units, LANES)), 0.0)
    table_ref[...] = jnp.sum(diagonal, axis=1, keepdims=True) / (nz * rows * GRID_LON)
    for share in shares:
        share.wait_send()
    out.wait()


def on_device(n, nz, ensemble, observation, valid_mask, band_start):
    held, variables, leads, rows, lon = ensemble.shape
    assert rows == n and rows % SUBLANES == 0
    units = variables * leads
    chunks = round_up(lon, LANES) // LANES
    group = round_up(units * chunks + 1, SUBLANES)
    pitch = held * group
    if pitch % 16 == 0:
        pitch += SUBLANES
    total = n * nz
    field, table = pl.pallas_call(
        functools.partial(kernel, n, nz),
        out_shape=(
            jax.ShapeDtypeStruct((variables, leads, rows // n, lon), jnp.float32),
            jax.ShapeDtypeStruct((units, 1), jnp.float32),
        ),
        in_specs=[
            pl.BlockSpec(memory_space=pl.ANY),
            pl.BlockSpec(memory_space=pl.ANY),
            pl.BlockSpec(memory_space=pltpu.SMEM),
            pl.BlockSpec(memory_space=pltpu.SMEM),
        ],
        out_specs=(
            pl.BlockSpec(memory_space=pl.ANY),
            pl.BlockSpec(memory_space=pltpu.VMEM),
        ),
        scratch_shapes=[
            pltpu.VMEM(ensemble.shape, jnp.float32),
            pltpu.VMEM(observation.shape, jnp.float32),
            pltpu.VMEM((n * pitch, LANES), jnp.float32),
            pltpu.VMEM((n * group, LANES), jnp.float32),
            pltpu.VMEM((n * held * group, LANES), jnp.float32),
            pltpu.VMEM((variables, leads, rows // n, lon), jnp.float32),
            pltpu.VMEM((total, LANES), jnp.float32),
            pltpu.SemaphoreType.DMA((held + 1,)),
            pltpu.SemaphoreType.DMA((n,)),
            pltpu.SemaphoreType.DMA((n,)),
            pltpu.SemaphoreType.DMA((total,)),
            pltpu.SemaphoreType.DMA((total,)),
        ],
        compiler_params=pltpu.CompilerParams(collective_id=0, has_side_effects=True),
        name="fair_crps",
    )(ensemble, observation, valid_mask, band_start)
    return field, table.reshape(variables, leads)


def solution(mesh):
    placed = (
        P("member", None, None, "lat", None),
        P(None, None, "lat", None),
        P("member"),
        P("lat"),
    )
    return jax.shard_map(
        functools.partial(on_device, mesh.shape["member"], mesh.shape["lat"]),
        mesh=mesh,
        in_specs=placed,
        out_specs=(P(None, None, ("lat", "member"), None), P()),
        check_vma=False,
    )
```

```python
import functools
import math

import jax
import jax.numpy as jnp
from jax import lax
from jax.experimental import pallas as pl
from jax.experimental.pallas import tpu as pltpu
from jax.sharding import PartitionSpec as P

GRID_LAT = 721
GRID_LON = 1440
LANES = 128
SUBLANES = 8
FILL = 1e30
VMEM_BYTES = 67_043_328 - 65_536
MESH = pl.DeviceIdType.MESH


def round_up(value, step):
    return (value + step - 1) // step * step


def sort_pairs(count):
    pairs = []
    p = 1
    while p < count:
        k = p
        while k >= 1:
            for j in range(k % p, count - k, 2 * k):
                for i in range(min(k, count - j - k)):
                    if (i + j) // (2 * p) == (i + j + k) // (2 * p):
                        pairs.append((i + j, i + j + k))
            k //= 2
        p *= 2
    return pairs


def other(me, k, n):
    partner, bit = 0, 1
    while bit < n:
        here = (me // bit) % 2
        partner = partner + bit * (1 - here if k & bit else here)
        bit *= 2
    return partner


class Packing:
    def __init__(self, units, lon):
        self.units, self.full, self.tail = units, lon // LANES, lon % LANES
        self.beside = LANES // self.tail if self.tail else 1
        self.tails = round_up(units, self.beside) // self.beside if self.tail else 0
        self.lines = units * self.full + self.tails

    def line(self, load, number):
        if number < self.units * self.full:
            return load(number // self.full, number % self.full * LANES, LANES)
        first = (number - self.units * self.full) * self.beside
        last = min(first + self.beside, self.units)
        parts = [load(u, self.full * LANES, self.tail) for u in range(first, last)]
        empty = LANES - self.tail * len(parts)
        if empty:
            parts.append(jnp.zeros((SUBLANES, empty), jnp.float32))
        return jnp.concatenate(parts, axis=1) if len(parts) > 1 else parts[0]

    def mask(self, unit, line, lane):
        inside = (line >= unit * self.full) & (line < (unit + 1) * self.full)
        if self.tail:
            low = unit % self.beside * self.tail
            at = self.units * self.full + unit // self.beside
            inside |= (line == at) & (lane >= low) & (lane < low + self.tail)
        return inside

    def pieces(self):
        for u in range(self.units):
            for c in range(self.full):
                yield u, c * LANES, LANES, u * self.full + c, 0
            if self.tail:
                at = self.units * self.full + u // self.beside
                yield u, self.full * LANES, self.tail, at, u % self.beside * self.tail


def kernel(
    n, nz, ens_ref, obs_ref, mask_ref, band_ref, field_ref, table_ref,
    ens_v, obs_v, mask_s, packet, obs_rows, gathered, partials,
    load_sem, send_sem, recv_sem, psend_sem, precv_sem, ready_sem,
):
    held, variables, leads, rows, lon = ens_ref.shape
    units = variables * leads
    packing = Packing(units, lon)
    lines = packing.lines
    pitch = packet.shape[0] // n
    stride = obs_rows.shape[0] // n
    slots = n * held
    total = n * nz
    me = lax.axis_index("member")
    band = lax.axis_index("lat")
    mine = band * n + me

    loads = [pltpu.make_async_copy(mask_ref, mask_s, load_sem.at[held + 1])]
    loads += [pltpu.make_async_copy(ens_ref.at[m], ens_v.at[m], load_sem.at[m]) for m in range(held)]
    loads.append(pltpu.make_async_copy(obs_ref, obs_v, load_sem.at[held]))
    for load in loads:
        load.start()

    plane = [{"member": other(me, k, n), "lat": band} for k in range(1, n)]
    line_peers = [{"member": me, "lat": lax.rem(band + k, nz)} for k in range(1, nz)]
    barrier = pltpu.get_barrier_semaphore()
    for peer in plane + line_peers:
        pl.semaphore_signal(barrier, inc=1, device_id=peer, device_id_type=MESH)

    loads[0].wait()
    for m in range(held):
        loads[1 + m].wait()
        flag = jnp.full((SUBLANES, LANES), mask_s[m], jnp.int32)
        keep = flag != 0
        for block in range(0, rows, SUBLANES):
            base = block * pitch

            def load(u, low, wide):
                return ens_v[m, u // leads, u % leads, pl.ds(block, SUBLANES), pl.ds(low, wide)]

            for line in range(lines):
                packet[pl.ds(base + m * lines + line, SUBLANES, stride=pitch), :] = jnp.where(
                    keep, packing.line(load, line), FILL
                )
            for line in range(held * lines + m, pitch, held):
                packet[pl.ds(base + line, SUBLANES, stride=pitch), :] = flag.astype(jnp.float32)

    pl.semaphore_wait(barrier, n - 1 + nz - 1)

    sends = []
    for k in sorted(range(1, n), key=lambda k: (-bin(k // 2).count("1"), k)):
        sends.append(
            pltpu.make_async_remote_copy(
                src_ref=packet.at[
                    pl.ds(pl.multiple_of(plane[k - 1]["member"] * pitch, SUBLANES), pitch)
                ],
                dst_ref=gathered.at[pl.ds(pl.multiple_of(me * pitch, SUBLANES), pitch)],
                send_sem=send_sem.at[k],
                recv_sem=recv_sem.at[k],
                device_id=plane[k - 1],
                device_id_type=MESH,
            )
        )
        sends[-1].start()
    for peer in line_peers:
        pl.semaphore_signal(ready_sem, inc=1, device_id=peer, device_id_type=MESH)

    loads[1 + held].wait()
    for block in range(0, rows, SUBLANES):

        def load(u, low, wide):
            return obs_v[u // leads, u % leads, pl.ds(block, SUBLANES), pl.ds(low, wide)]

        for line in range(lines):
            obs_rows[pl.ds(block * stride + line, SUBLANES, stride=stride), :] = packing.line(
                load, line
            )
    gathered[pl.ds(pl.multiple_of(me * pitch, SUBLANES), pitch), :] = packet[
        pl.ds(pl.multiple_of(me * pitch, SUBLANES), pitch), :
    ]
    row_number = jnp.full((1, LANES), band_ref[0] + me, jnp.int32).astype(jnp.float32)
    weight = jnp.cos((90.0 - row_number * 180.0 / (GRID_LAT - 1)) * math.pi / 180.0)
    pl.semaphore_wait(ready_sem, nz - 1)

    for send in sends:
        send.wait_recv()

    flags = jnp.concatenate(
        [gathered[pl.ds(d * pitch + held * lines, held), :] for d in range(n)], axis=0
    )
    count = jnp.broadcast_to(jnp.sum(flags, axis=0, keepdims=True), (SUBLANES, LANES))
    per_one = 1.0 / count
    per_pair = per_one / (count - 1.0)
    skill_weight, spread_weight = [], []
    for i in range(slots):
        counted = i < count
        skill_weight.append(jnp.where(counted, per_one, 0.0))
        spread_weight.append(jnp.where(counted, (2.0 * i + 1.0 - count) * per_pair, 0.0))

    network = sort_pairs(slots)
    sums = [None] * units
    blocks = []
    lane = lax.broadcasted_iota(jnp.int32, (SUBLANES, LANES), 1)
    for j in range(0, lines, SUBLANES):
        x = [
            gathered[pl.ds(s // held * pitch + s % held * lines + j, SUBLANES), :]
            for s in range(slots)
        ]
        for a, b in network:
            x[a], x[b] = jnp.minimum(x[a], x[b]), jnp.maximum(x[a], x[b])
        truth = obs_rows[pl.ds(pl.multiple_of(me * stride + j, SUBLANES), SUBLANES), :]
        score = None
        for i in range(slots):
            term = skill_weight[i] * jnp.abs(x[i] - truth) - spread_weight[i] * x[i]
            score = term if score is None else score + term
        blocks.append(score)
        line = j + lax.broadcasted_iota(jnp.int32, (SUBLANES, LANES), 0)
        for u in range(units):
            part = jnp.where(packing.mask(u, line, lane), score, 0.0)
            sums[u] = part if sums[u] is None else sums[u] + part

    lane = lax.broadcasted_iota(jnp.int32, (1, LANES), 1)
    row = jnp.zeros((1, LANES), jnp.float32)
    for u in range(units):
        one = jnp.sum(jnp.sum(sums[u], axis=0, keepdims=True), axis=1, keepdims=True)
        row = jnp.where(lane == u, one, row)
    partials[pl.ds(mine, 1), :] = row * weight

    for send in sends:
        send.wait_send()

    def share_with(far):
        return pltpu.make_async_remote_copy(
            src_ref=partials.at[pl.ds(mine, 1)],
            dst_ref=partials.at[pl.ds(mine, 1)],
            send_sem=psend_sem.at[far],
            recv_sem=precv_sem.at[mine],
            device_id={"member": far % n, "lat": far // n},
            device_id_type=MESH,
        )

    def share_from(far):
        return pltpu.make_async_remote_copy(
            src_ref=partials.at[pl.ds(mine, 1)],
            dst_ref=partials.at[pl.ds(far, 1)],
            send_sem=psend_sem.at[far],
            recv_sem=precv_sem.at[far],
            device_id={"member": far % n, "lat": far // n},
            device_id_type=MESH,
        )

    for far in range(total):
        pl.when(far != mine)(lambda far=far: share_with(far).start())

    for u, low, wide, at, first in packing.pieces():
        piece = blocks[at // SUBLANES][at % SUBLANES : at % SUBLANES + 1, first : first + wide]
        field_ref[u // leads, u % leads, :, pl.ds(low, wide)] = piece

    for far in range(total):
        pl.when(far != mine)(lambda far=far: share_from(far).wait_recv())
    summed = jnp.sum(partials[...], axis=0, keepdims=True)
    table_ref[...] = summed[:, :units] / (nz * rows * GRID_LON)
    for far in range(total):
        pl.when(far != mine)(lambda far=far: share_with(far).wait_send())


def on_device(n, nz, ensemble, observation, valid_mask, band_start):
    held, variables, leads, rows, lon = ensemble.shape
    assert rows == n and rows % SUBLANES == 0
    units = variables * leads
    packing = Packing(units, lon)
    pitch = round_up(held * packing.lines + held, SUBLANES)
    stride = round_up(packing.lines, SUBLANES)
    total = n * nz
    field, table = pl.pallas_call(
        functools.partial(kernel, n, nz),
        out_shape=(
            pltpu.VMEM((variables, leads, rows // n, lon), jnp.float32),
            pltpu.VMEM((1, units), jnp.float32),
        ),
        in_specs=[pl.BlockSpec(memory_space=pltpu.HBM)] * 3 + [pl.BlockSpec(memory_space=pltpu.SMEM)],
        out_specs=(
            pl.BlockSpec(memory_space=pltpu.VMEM),
            pl.BlockSpec(memory_space=pltpu.VMEM),
        ),
        scratch_shapes=[
            pltpu.VMEM(ensemble.shape, jnp.float32),
            pltpu.VMEM(observation.shape, jnp.float32),
            pltpu.SMEM(valid_mask.shape, jnp.int32),
            pltpu.VMEM((n * pitch, LANES), jnp.float32),
            pltpu.VMEM((n * stride, LANES), jnp.float32),
            pltpu.VMEM((n * pitch + SUBLANES, LANES), jnp.float32),
            pltpu.VMEM((total, LANES), jnp.float32),
            pltpu.SemaphoreType.DMA((held + 2,)),
            pltpu.SemaphoreType.DMA((n,)),
            pltpu.SemaphoreType.DMA((n,)),
            pltpu.SemaphoreType.DMA((total,)),
            pltpu.SemaphoreType.DMA((total,)),
            pltpu.SemaphoreType.REGULAR,
        ],
        compiler_params=pltpu.CompilerParams(
            collective_id=0, has_side_effects=True, vmem_limit_bytes=VMEM_BYTES
        ),
        name="fair_crps",
    )(ensemble, observation, valid_mask, band_start)
    return field, table.reshape(variables, leads)


def solution(mesh):
    placed = (
        P("member", None, None, "lat", None),
        P(None, None, "lat", None),
        P("member"),
        P("lat"),
    )
    return jax.shard_map(
        functools.partial(on_device, mesh.shape["member"], mesh.shape["lat"]),
        mesh=mesh,
        in_specs=placed,
        out_specs=(P(None, None, ("lat", "member"), None), P()),
        check_vma=False,
    )
```

```python
import functools
import math

import jax
import jax.numpy as jnp
from jax import lax
from jax.experimental import pallas as pl
from jax.experimental.pallas import tpu as pltpu
from jax.sharding import PartitionSpec as P

GRID_LAT = 721
GRID_LON = 1440
LANES = 128
SUBLANES = 8
FILL = 1e30
VMEM_BYTES = 67_043_328 - 65_536
MESH = pl.DeviceIdType.MESH


def round_up(value, step):
    return (value + step - 1) // step * step


def sort_pairs(count):
    pairs = []
    p = 1
    while p < count:
        k = p
        while k >= 1:
            for j in range(k % p, count - k, 2 * k):
                for i in range(min(k, count - j - k)):
                    if (i + j) // (2 * p) == (i + j + k) // (2 * p):
                        pairs.append((i + j, i + j + k))
            k //= 2
        p *= 2
    return pairs


def other(me, k, n):
    partner, bit = 0, 1
    while bit < n:
        here = (me // bit) % 2
        partner = partner + bit * (1 - here if k & bit else here)
        bit *= 2
    return partner


class Packing:
    def __init__(self, units, lon):
        self.units, self.full, self.tail = units, lon // LANES, lon % LANES
        self.beside = LANES // self.tail if self.tail else 1
        self.tails = round_up(units, self.beside) // self.beside if self.tail else 0
        self.lines = units * self.full + self.tails

    def line(self, load, number):
        if number < self.units * self.full:
            return load(number // self.full, number % self.full * LANES, LANES)
        first = (number - self.units * self.full) * self.beside
        last = min(first + self.beside, self.units)
        parts = [load(u, self.full * LANES, self.tail) for u in range(first, last)]
        empty = LANES - self.tail * len(parts)
        if empty:
            parts.append(jnp.zeros((SUBLANES, empty), jnp.float32))
        return jnp.concatenate(parts, axis=1) if len(parts) > 1 else parts[0]

    def mask(self, unit, line, lane):
        inside = (line >= unit * self.full) & (line < (unit + 1) * self.full)
        if self.tail:
            low = unit % self.beside * self.tail
            at = self.units * self.full + unit // self.beside
            inside |= (line == at) & (lane >= low) & (lane < low + self.tail)
        return inside

    def pieces(self):
        for u in range(self.units):
            for c in range(self.full):
                yield u, c * LANES, LANES, u * self.full + c, 0
            if self.tail:
                at = self.units * self.full + u // self.beside
                yield u, self.full * LANES, self.tail, at, u % self.beside * self.tail


def kernel(
    n, nz, ens_ref, obs_ref, mask_ref, band_ref, field_ref, table_ref,
    ens_v, obs_v, mask_s, packet, obs_rows, gathered, partials,
    load_sem, send_sem, recv_sem, psend_sem, precv_sem, ready_sem,
):
    held, variables, leads, rows, lon = ens_ref.shape
    units = variables * leads
    packing = Packing(units, lon)
    lines = packing.lines
    pitch = packet.shape[0] // n
    stride = obs_rows.shape[0] // n
    slots = n * held
    total = n * nz
    me = lax.axis_index("member")
    band = lax.axis_index("lat")
    mine = band * n + me

    loads = [pltpu.make_async_copy(mask_ref, mask_s, load_sem.at[held + 1])]
    loads += [pltpu.make_async_copy(ens_ref.at[m], ens_v.at[m], load_sem.at[m]) for m in range(held)]
    loads.append(pltpu.make_async_copy(obs_ref, obs_v, load_sem.at[held]))
    plane = [{"member": other(me, k, n), "lat": band} for k in range(1, n)]
    line_peers = [{"member": me, "lat": lax.rem(band + k, nz)} for k in range(1, nz)]
    barrier = pltpu.get_barrier_semaphore()
    for peer in plane[::-1] + line_peers:
        pl.semaphore_signal(barrier, inc=1, device_id=peer, device_id_type=MESH)
    for load in loads:
        load.start()

    loads[0].wait()
    for m in range(held):
        loads[1 + m].wait()
        flag = jnp.full((SUBLANES, LANES), mask_s[m], jnp.int32)
        keep = flag != 0
        for block in range(0, rows, SUBLANES):
            base = block * pitch

            def load(u, low, wide):
                return ens_v[m, u // leads, u % leads, pl.ds(block, SUBLANES), pl.ds(low, wide)]

            for line in range(lines):
                packet[pl.ds(base + m * lines + line, SUBLANES, stride=pitch), :] = jnp.where(
                    keep, packing.line(load, line), FILL
                )
            for line in range(held * lines + m, pitch, held):
                packet[pl.ds(base + line, SUBLANES, stride=pitch), :] = flag.astype(jnp.float32)

    pl.semaphore_wait(barrier, n - 1 + nz - 1)

    sends = []
    for k in sorted(range(1, n), key=lambda k: (-bin(k // 2).count("1"), k)):
        sends.append(
            pltpu.make_async_remote_copy(
                src_ref=packet.at[
                    pl.ds(pl.multiple_of(plane[k - 1]["member"] * pitch, SUBLANES), pitch)
                ],
                dst_ref=gathered.at[pl.ds(pl.multiple_of(me * pitch, SUBLANES), pitch)],
                send_sem=send_sem.at[k],
                recv_sem=recv_sem.at[k],
                device_id=plane[k - 1],
                device_id_type=MESH,
            )
        )
        sends[-1].start()
    for peer in line_peers:
        pl.semaphore_signal(ready_sem, inc=1, device_id=peer, device_id_type=MESH)

    loads[1 + held].wait()
    for block in range(0, rows, SUBLANES):

        def load(u, low, wide):
            return obs_v[u // leads, u % leads, pl.ds(block, SUBLANES), pl.ds(low, wide)]

        for line in range(lines):
            obs_rows[pl.ds(block * stride + line, SUBLANES, stride=stride), :] = packing.line(
                load, line
            )
    gathered[pl.ds(pl.multiple_of(me * pitch, SUBLANES), pitch), :] = packet[
        pl.ds(pl.multiple_of(me * pitch, SUBLANES), pitch), :
    ]
    row_number = jnp.full((1, LANES), band_ref[0] + me, jnp.int32).astype(jnp.float32)
    weight = jnp.cos((90.0 - row_number * 180.0 / (GRID_LAT - 1)) * math.pi / 180.0)
    pl.semaphore_wait(ready_sem, nz - 1)

    for send in sends:
        send.wait_recv()

    flags = jnp.concatenate(
        [gathered[pl.ds(d * pitch + held * lines, held), :] for d in range(n)], axis=0
    )
    count = jnp.broadcast_to(jnp.sum(flags, axis=0, keepdims=True), (SUBLANES, LANES))
    per_one = 1.0 / count
    per_pair = per_one / (count - 1.0)
    skill_weight, spread_weight = [], []
    for i in range(slots):
        counted = i < count
        skill_weight.append(jnp.where(counted, per_one, 0.0))
        spread_weight.append(jnp.where(counted, (2.0 * i + 1.0 - count) * per_pair, 0.0))

    network = sort_pairs(slots)
    sums = [None] * units
    blocks = []
    lane = lax.broadcasted_iota(jnp.int32, (SUBLANES, LANES), 1)
    for j in range(0, lines, SUBLANES):
        x = [
            gathered[pl.ds(s // held * pitch + s % held * lines + j, SUBLANES), :]
            for s in range(slots)
        ]
        for a, b in network:
            x[a], x[b] = jnp.minimum(x[a], x[b]), jnp.maximum(x[a], x[b])
        truth = obs_rows[pl.ds(pl.multiple_of(me * stride + j, SUBLANES), SUBLANES), :]
        score = None
        for i in range(slots):
            term = skill_weight[i] * jnp.abs(x[i] - truth) - spread_weight[i] * x[i]
            score = term if score is None else score + term
        blocks.append(score)
        line = j + lax.broadcasted_iota(jnp.int32, (SUBLANES, LANES), 0)
        for u in range(units):
            part = jnp.where(packing.mask(u, line, lane), score, 0.0)
            sums[u] = part if sums[u] is None else sums[u] + part

    lane = lax.broadcasted_iota(jnp.int32, (1, LANES), 1)
    row = jnp.zeros((1, LANES), jnp.float32)
    for u in range(units):
        one = jnp.sum(jnp.sum(sums[u], axis=0, keepdims=True), axis=1, keepdims=True)
        row = jnp.where(lane == u, one, row)
    partials[pl.ds(mine, 1), :] = row * weight

    for send in sends:
        send.wait_send()

    def share_with(far):
        return pltpu.make_async_remote_copy(
            src_ref=partials.at[pl.ds(mine, 1)],
            dst_ref=partials.at[pl.ds(mine, 1)],
            send_sem=psend_sem.at[far],
            recv_sem=precv_sem.at[mine],
            device_id={"member": far % n, "lat": far // n},
            device_id_type=MESH,
        )

    def share_from(far):
        return pltpu.make_async_remote_copy(
            src_ref=partials.at[pl.ds(mine, 1)],
            dst_ref=partials.at[pl.ds(far, 1)],
            send_sem=psend_sem.at[far],
            recv_sem=precv_sem.at[far],
            device_id={"member": far % n, "lat": far // n},
            device_id_type=MESH,
        )

    for far in range(total):
        pl.when(far != mine)(lambda far=far: share_with(far).start())

    for u, low, wide, at, first in packing.pieces():
        piece = blocks[at // SUBLANES][at % SUBLANES : at % SUBLANES + 1, first : first + wide]
        field_ref[u // leads, u % leads, :, pl.ds(low, wide)] = piece

    for far in range(total):
        pl.when(far != mine)(lambda far=far: share_from(far).wait_recv())
    summed = jnp.sum(partials[...], axis=0, keepdims=True)
    table_ref[...] = summed[:, :units] / (nz * rows * GRID_LON)
    for far in range(total):
        pl.when(far != mine)(lambda far=far: share_with(far).wait_send())


def write_out(field_ref, table_ref, field_out, table_out, sem):
    copies = [
        pltpu.make_async_copy(field_ref, field_out, sem.at[0]),
        pltpu.make_async_copy(table_ref, table_out, sem.at[1]),
    ]
    for copy in copies:
        copy.start()
    for copy in copies:
        copy.wait()


def on_device(n, nz, ensemble, observation, valid_mask, band_start):
    held, variables, leads, rows, lon = ensemble.shape
    assert rows == n and rows % SUBLANES == 0
    units = variables * leads
    packing = Packing(units, lon)
    pitch = round_up(held * packing.lines + held, SUBLANES)
    stride = round_up(packing.lines, SUBLANES)
    total = n * nz
    field, table = pl.pallas_call(
        functools.partial(kernel, n, nz),
        out_shape=(
            pltpu.VMEM((variables, leads, rows // n, lon), jnp.float32),
            pltpu.VMEM((1, units), jnp.float32),
        ),
        in_specs=[pl.BlockSpec(memory_space=pltpu.HBM)] * 3 + [pl.BlockSpec(memory_space=pltpu.SMEM)],
        out_specs=(
            pl.BlockSpec(memory_space=pltpu.VMEM),
            pl.BlockSpec(memory_space=pltpu.VMEM),
        ),
        scratch_shapes=[
            pltpu.VMEM(ensemble.shape, jnp.float32),
            pltpu.VMEM(observation.shape, jnp.float32),
            pltpu.SMEM(valid_mask.shape, jnp.int32),
            pltpu.VMEM((n * pitch, LANES), jnp.float32),
            pltpu.VMEM((n * stride, LANES), jnp.float32),
            pltpu.VMEM((n * pitch + SUBLANES, LANES), jnp.float32),
            pltpu.VMEM((total, LANES), jnp.float32),
            pltpu.SemaphoreType.DMA((held + 2,)),
            pltpu.SemaphoreType.DMA((n,)),
            pltpu.SemaphoreType.DMA((n,)),
            pltpu.SemaphoreType.DMA((total,)),
            pltpu.SemaphoreType.DMA((total,)),
            pltpu.SemaphoreType.REGULAR,
        ],
        compiler_params=pltpu.CompilerParams(
            collective_id=0, has_side_effects=True, vmem_limit_bytes=VMEM_BYTES
        ),
        name="fair_crps",
    )(ensemble, observation, valid_mask, band_start)
    field, table = pl.pallas_call(
        write_out,
        out_shape=(
            jax.ShapeDtypeStruct(field.shape, jnp.float32),
            jax.ShapeDtypeStruct(table.shape, jnp.float32),
        ),
        in_specs=[pl.BlockSpec(memory_space=pltpu.VMEM)] * 2,
        out_specs=(pl.BlockSpec(memory_space=pltpu.HBM),) * 2,
        scratch_shapes=[pltpu.SemaphoreType.DMA((2,))],
        name="write_out",
    )(*(pltpu.with_memory_space_constraint(a, pltpu.VMEM) for a in (field, table)))
    return field, table.reshape(variables, leads)


def solution(mesh):
    placed = (
        P("member", None, None, "lat", None),
        P(None, None, "lat", None),
        P("member"),
        P("lat"),
    )
    return jax.shard_map(
        functools.partial(on_device, mesh.shape["member"], mesh.shape["lat"]),
        mesh=mesh,
        in_specs=placed,
        out_specs=(P(None, None, ("lat", "member"), None), P()),
        check_vma=False,
    )
```

```python
import functools
import math

import jax
import jax.numpy as jnp
from jax import lax
from jax.experimental import pallas as pl
from jax.experimental.pallas import tpu as pltpu
from jax.sharding import PartitionSpec as P

GRID_LAT = 721
GRID_LON = 1440
LANES = 128
SUBLANES = 8
FILL = 1e30
VMEM_BYTES = 67_043_328 - 65_536
MESH = pl.DeviceIdType.MESH


def round_up(value, step):
    return (value + step - 1) // step * step


def sort_pairs(count):
    pairs = []
    p = 1
    while p < count:
        k = p
        while k >= 1:
            for j in range(k % p, count - k, 2 * k):
                for i in range(min(k, count - j - k)):
                    if (i + j) // (2 * p) == (i + j + k) // (2 * p):
                        pairs.append((i + j, i + j + k))
            k //= 2
        p *= 2
    return pairs


def other(me, k, n):
    partner, bit = 0, 1
    while bit < n:
        here = (me // bit) % 2
        partner = partner + bit * (1 - here if k & bit else here)
        bit *= 2
    return partner


class Packing:
    def __init__(self, units, lon):
        self.units, self.full, self.tail = units, lon // LANES, lon % LANES
        self.beside = LANES // self.tail if self.tail else 1
        self.tails = round_up(units, self.beside) // self.beside if self.tail else 0
        self.lines = units * self.full + self.tails
        self.used = (units - 1) % self.beside * self.tail + self.tail

    def line(self, load, number):
        if number < self.units * self.full:
            return load(number // self.full, number % self.full * LANES, LANES)
        first = (number - self.units * self.full) * self.beside
        last = min(first + self.beside, self.units)
        parts = [load(u, self.full * LANES, self.tail) for u in range(first, last)]
        empty = LANES - self.tail * len(parts)
        if empty:
            parts.append(jnp.zeros((SUBLANES, empty), jnp.float32))
        return jnp.concatenate(parts, axis=1) if len(parts) > 1 else parts[0]

    def mask(self, unit, line, lane):
        inside = (line >= unit * self.full) & (line < (unit + 1) * self.full)
        if self.tail:
            low = unit % self.beside * self.tail
            at = self.units * self.full + unit // self.beside
            inside |= (line == at) & (lane >= low) & (lane < low + self.tail)
        return inside

    def pieces(self):
        for u in range(self.units):
            for c in range(self.full):
                yield u, c * LANES, LANES, u * self.full + c, 0
            if self.tail:
                at = self.units * self.full + u // self.beside
                yield u, self.full * LANES, self.tail, at, u % self.beside * self.tail


def kernel(
    n, nz, ens_ref, obs_ref, mask_ref, band_ref, field_ref, table_ref,
    ens_v, obs_v, mask_s, packet, obs_rows, gathered, partials,
    load_sem, send_sem, recv_sem, psend_sem, precv_sem, ready_sem,
):
    held, variables, leads, rows, lon = ens_ref.shape
    units = variables * leads
    packing = Packing(units, lon)
    lines = packing.lines
    pitch = packet.shape[0] // n
    stride = obs_rows.shape[0] // n
    slots = n * held
    total = n * nz
    me = lax.axis_index("member")
    band = lax.axis_index("lat")
    mine = band * n + me

    loads = [pltpu.make_async_copy(mask_ref, mask_s, load_sem.at[held + 1])]
    loads += [pltpu.make_async_copy(ens_ref.at[m], ens_v.at[m], load_sem.at[m]) for m in range(held)]
    loads.append(pltpu.make_async_copy(obs_ref, obs_v, load_sem.at[held]))
    plane = [{"member": other(me, k, n), "lat": band} for k in range(1, n)]
    line_peers = [{"member": me, "lat": lax.rem(band + k, nz)} for k in range(1, nz)]
    barrier = pltpu.get_barrier_semaphore()
    for peer in plane[::-1] + line_peers:
        pl.semaphore_signal(barrier, inc=1, device_id=peer, device_id_type=MESH)
    for load in loads:
        load.start()

    loads[0].wait()
    free = lax.broadcasted_iota(jnp.int32, (SUBLANES, LANES), 1) >= packing.used
    for m in range(held):
        loads[1 + m].wait()
        flag = jnp.full((SUBLANES, LANES), mask_s[m], jnp.int32)
        keep = flag != 0
        for block in range(0, rows, SUBLANES):
            base = block * pitch

            def load(u, low, wide):
                return ens_v[m, u // leads, u % leads, pl.ds(block, SUBLANES), pl.ds(low, wide)]

            for line in range(lines):
                value = jnp.where(keep, packing.line(load, line), FILL)
                if line == lines - 1:
                    value = jnp.where(free, flag.astype(jnp.float32), value)
                packet[pl.ds(base + m * lines + line, SUBLANES, stride=pitch), :] = value
            for line in range(held * lines + m, pitch, held):
                packet[pl.ds(base + line, SUBLANES, stride=pitch), :] = jnp.zeros_like(value)

    pl.semaphore_wait(barrier, n - 1 + nz - 1)

    sends = []
    for k in sorted(range(1, n), key=lambda k: (-bin(k // 2).count("1"), k)):
        sends.append(
            pltpu.make_async_remote_copy(
                src_ref=packet.at[
                    pl.ds(pl.multiple_of(plane[k - 1]["member"] * pitch, SUBLANES), held * lines)
                ],
                dst_ref=gathered.at[
                    pl.ds(pl.multiple_of(me * pitch, SUBLANES), held * lines)
                ],
                send_sem=send_sem.at[k],
                recv_sem=recv_sem.at[k],
                device_id=plane[k - 1],
                device_id_type=MESH,
            )
        )
        sends[-1].start()
    for peer in line_peers:
        pl.semaphore_signal(ready_sem, inc=1, device_id=peer, device_id_type=MESH)

    loads[1 + held].wait()
    for block in range(0, rows, SUBLANES):

        def load(u, low, wide):
            return obs_v[u // leads, u % leads, pl.ds(block, SUBLANES), pl.ds(low, wide)]

        for line in range(lines):
            obs_rows[pl.ds(block * stride + line, SUBLANES, stride=stride), :] = packing.line(
                load, line
            )
    gathered[pl.ds(pl.multiple_of(me * pitch, SUBLANES), pitch), :] = packet[
        pl.ds(pl.multiple_of(me * pitch, SUBLANES), pitch), :
    ]
    row_number = jnp.full((1, LANES), band_ref[0] + me, jnp.int32).astype(jnp.float32)
    weight = jnp.cos((90.0 - row_number * 180.0 / (GRID_LAT - 1)) * math.pi / 180.0)
    pl.semaphore_wait(ready_sem, nz - 1)

    for send in sends:
        send.wait_recv()

    flags = jnp.concatenate(
        [
            gathered[pl.ds(s // held * pitch + s % held * lines + lines - 1, 1), :]
            for s in range(slots)
        ],
        axis=0,
    )
    count = jnp.sum(flags, axis=0, keepdims=True)
    count = jnp.where(free[:1], count, 0.0)
    count = jnp.max(count, axis=1, keepdims=True)
    count = jnp.broadcast_to(count, (SUBLANES, LANES))
    per_one = 1.0 / count
    per_pair = per_one / (count - 1.0)
    skill_weight, spread_weight = [], []
    for i in range(slots):
        counted = i < count
        skill_weight.append(jnp.where(counted, per_one, 0.0))
        spread_weight.append(jnp.where(counted, (2.0 * i + 1.0 - count) * per_pair, 0.0))

    network = sort_pairs(slots)
    sums = [None] * units
    blocks = []
    lane = lax.broadcasted_iota(jnp.int32, (SUBLANES, LANES), 1)
    for j in range(0, lines, SUBLANES):
        x = [
            gathered[pl.ds(s // held * pitch + s % held * lines + j, SUBLANES), :]
            for s in range(slots)
        ]
        for a, b in network:
            x[a], x[b] = jnp.minimum(x[a], x[b]), jnp.maximum(x[a], x[b])
        truth = obs_rows[pl.ds(pl.multiple_of(me * stride + j, SUBLANES), SUBLANES), :]
        score = None
        for i in range(slots):
            term = skill_weight[i] * jnp.abs(x[i] - truth) - spread_weight[i] * x[i]
            score = term if score is None else score + term
        blocks.append(score)
        line = j + lax.broadcasted_iota(jnp.int32, (SUBLANES, LANES), 0)
        for u in range(units):
            part = jnp.where(packing.mask(u, line, lane), score, 0.0)
            sums[u] = part if sums[u] is None else sums[u] + part

    lane = lax.broadcasted_iota(jnp.int32, (1, LANES), 1)
    row = jnp.zeros((1, LANES), jnp.float32)
    for u in range(units):
        one = jnp.sum(jnp.sum(sums[u], axis=0, keepdims=True), axis=1, keepdims=True)
        row = jnp.where(lane == u, one, row)
    partials[pl.ds(mine, 1), :] = row * weight

    def share_with(far):
        return pltpu.make_async_remote_copy(
            src_ref=partials.at[pl.ds(mine, 1)],
            dst_ref=partials.at[pl.ds(mine, 1)],
            send_sem=psend_sem.at[far],
            recv_sem=precv_sem.at[mine],
            device_id={"member": far % n, "lat": far // n},
            device_id_type=MESH,
        )

    def share_from(far):
        return pltpu.make_async_remote_copy(
            src_ref=partials.at[pl.ds(mine, 1)],
            dst_ref=partials.at[pl.ds(far, 1)],
            send_sem=psend_sem.at[far],
            recv_sem=precv_sem.at[far],
            device_id={"member": far % n, "lat": far // n},
            device_id_type=MESH,
        )

    for far in range(total):
        pl.when(far != mine)(lambda far=far: share_with(far).start())

    for u, low, wide, at, first in packing.pieces():
        piece = blocks[at // SUBLANES][at % SUBLANES : at % SUBLANES + 1, first : first + wide]
        field_ref[u // leads, u % leads, :, pl.ds(low, wide)] = piece

    for send in sends:
        send.wait_send()
    for far in range(total):
        pl.when(far != mine)(lambda far=far: share_with(far).wait_send())
    for far in range(total):
        pl.when(far != mine)(lambda far=far: share_from(far).wait_recv())
    summed = jnp.sum(partials[...], axis=0, keepdims=True)
    table_ref[...] = summed[:, :units] / (nz * rows * GRID_LON)


def write_out(field_ref, table_ref, field_out, table_out, sem):
    copies = [
        pltpu.make_async_copy(field_ref, field_out, sem.at[0]),
        pltpu.make_async_copy(table_ref, table_out, sem.at[1]),
    ]
    for copy in copies:
        copy.start()
    for copy in copies:
        copy.wait()


def on_device(n, nz, ensemble, observation, valid_mask, band_start):
    held, variables, leads, rows, lon = ensemble.shape
    assert rows == n and rows % SUBLANES == 0
    units = variables * leads
    packing = Packing(units, lon)
    assert packing.tails and packing.used < LANES
    pitch = round_up(held * packing.lines, SUBLANES)
    stride = round_up(packing.lines, SUBLANES)
    total = n * nz
    field, table = pl.pallas_call(
        functools.partial(kernel, n, nz),
        out_shape=(
            pltpu.VMEM((variables, leads, rows // n, lon), jnp.float32),
            pltpu.VMEM((1, units), jnp.float32),
        ),
        in_specs=[pl.BlockSpec(memory_space=pltpu.HBM)] * 3 + [pl.BlockSpec(memory_space=pltpu.SMEM)],
        out_specs=(
            pl.BlockSpec(memory_space=pltpu.VMEM),
            pl.BlockSpec(memory_space=pltpu.VMEM),
        ),
        scratch_shapes=[
            pltpu.VMEM(ensemble.shape, jnp.float32),
            pltpu.VMEM(observation.shape, jnp.float32),
            pltpu.SMEM(valid_mask.shape, jnp.int32),
            pltpu.VMEM((n * pitch, LANES), jnp.float32),
            pltpu.VMEM((n * stride, LANES), jnp.float32),
            pltpu.VMEM((n * pitch + SUBLANES, LANES), jnp.float32),
            pltpu.VMEM((total, LANES), jnp.float32),
            pltpu.SemaphoreType.DMA((held + 2,)),
            pltpu.SemaphoreType.DMA((n,)),
            pltpu.SemaphoreType.DMA((n,)),
            pltpu.SemaphoreType.DMA((total,)),
            pltpu.SemaphoreType.DMA((total,)),
            pltpu.SemaphoreType.REGULAR,
        ],
        compiler_params=pltpu.CompilerParams(
            collective_id=0, has_side_effects=True, vmem_limit_bytes=VMEM_BYTES
        ),
        name="fair_crps",
    )(ensemble, observation, valid_mask, band_start)
    field, table = pl.pallas_call(
        write_out,
        out_shape=(
            jax.ShapeDtypeStruct(field.shape, jnp.float32),
            jax.ShapeDtypeStruct(table.shape, jnp.float32),
        ),
        in_specs=[pl.BlockSpec(memory_space=pltpu.VMEM)] * 2,
        out_specs=(pl.BlockSpec(memory_space=pltpu.HBM),) * 2,
        scratch_shapes=[pltpu.SemaphoreType.DMA((2,))],
        name="write_out",
    )(*(pltpu.with_memory_space_constraint(a, pltpu.VMEM) for a in (field, table)))
    return field, table.reshape(variables, leads)


def solution(mesh):
    placed = (
        P("member", None, None, "lat", None),
        P(None, None, "lat", None),
        P("member"),
        P("lat"),
    )
    return jax.shard_map(
        functools.partial(on_device, mesh.shape["member"], mesh.shape["lat"]),
        mesh=mesh,
        in_specs=placed,
        out_specs=(P(None, None, ("lat", "member"), None), P()),
        check_vma=False,
    )
```
